768 devices in a mesh: dp: 24 (over z, y_lo), group: 32 (over x, y_hi, core).
Axes of the slice: x: 4, y: 8 (y_hi: 4, y_lo: 2; y = y_hi * 2 + y_lo), z: 12, core: 2. Of those that a mesh axis runs over, the one named last changes fastest.
Arguments:
- query: bfloat16 [98304, 4096], P(('dp', 'group')), may hold values from -6 to 6
- comp_key: bfloat16 [98304, 512], P(('dp', 'group')), may hold values from -6 to 6
- comp_value: bfloat16 [98304, 512], P(('dp', 'group')), may hold values from -6 to 6
- prompt_key: bfloat16 [3072, 512], P(('dp', 'group')), may hold values from -6 to 6
- prompt_value: bfloat16 [3072, 512], P(('dp', 'group')), may hold values from -6 to 6
- d_out: bfloat16 [98304, 4096], P(('dp', 'group')), may hold values from -6 to 6
- q_gain: float32 [128], replicated, may hold values from 0.5 to 1.5
- k_gain: float32 [128], replicated, may hold values from 0.5 to 1.5
- lengths: int32 [768], P(('dp', 'group')), may hold values from 1 to 128, 61440 in all
Outputs:
- d_query: bfloat16 [98304, 4096], P(('dp', 'group'))
- d_comp_key: bfloat16 [98304, 512], P(('dp', 'group'))
- d_comp_value: bfloat16 [98304, 512], P(('dp', 'group'))
- d_prompt_key: bfloat16 [3072, 512], P(('dp', 'group'))
- d_prompt_value: bfloat16 [3072, 512], P(('dp', 'group'))
- d_q_gain: float32 [128], replicated
- d_k_gain: float32 [128], replicated
The draws below stay inside these ranges and needn't reach their ends.
Inputs may be any that keep to these rules, and one draw needn't show every extreme that they name: `lengths`: each entry is the live slots of one completion, at most 128; some completion has exactly 128.
All inputs are finite; a program needn't handle non-finite values. No bound on the sum of `lengths` on one device may be relied on, other than what follows from the above.
Results may differ from the reference program's by a relative error of at most 0.025.
Values may be sent and summed in bfloat16 or wider, within the bound.
No kernel may reach another device: no remote copies, remote signals or barrier semaphores. Data moves between devices by JAX's collectives and lax.ppermute only.
A program may use at most 64 MiB of HBM per device.

```python
import math
import jax
import jax.numpy as jnp
import numpy as np
from jax import lax

HD = 128
HQ = 32
HK = 4
C_DEV = 128
PROMPT = 128
SAMPLES = 768
COMP_TOK = 98304
PROMPT_TOK = 3072
N_DP = 24
N_GROUP = 32


def block_levels(key, extent, cuts, least, top_value):
    loudness = 1.0
    for dim, blocks in cuts:
        draws = jax.random.uniform(jax.random.fold_in(jax.random.fold_in(key, 6), dim), (blocks,), jnp.float32, least / len(cuts), top_value / len(cuts))
        loudness = loudness * jnp.repeat(jnp.exp(draws), extent[dim] // blocks).reshape((-1,) + (1,) * (len(extent) - 1 - dim))
    return loudness


def profile(number_of, total, bound, skew):
    loads = [(1 << 20) // math.isqrt(grade ** skew) + 1 for grade in range(2, number_of + 1)]
    spare, counts = total - bound - (number_of - 1), [1] * (number_of - 1)
    while spare > 0:
        free = [i for i in range(number_of - 1) if counts[i] < bound]
        mass, left = sum([loads[i] for i in free]), spare
        for i in free:
            addition = min(bound - counts[i], max(1, left * loads[i] // mass), spare)
            counts[i] = counts[i] + addition
            spare = spare - addition
    return np.array([bound] + counts)


def ragged_sizes(own_key, amount, total, bound, lean):
    if amount == 2:
        one = jax.random.randint(own_key, (), max(1, total - bound), min(bound, total - 1) + 1)
        return jnp.stack([one, total - one])
    sizes = jnp.asarray(profile(amount, total, bound, lean), jnp.int32)
    couples = (amount - 1) // 2
    giver, sink = sizes[1:1 + 2 * couples:2], sizes[2:2 + 2 * couples:2]
    slack = jnp.minimum(giver - 1, bound - sink)
    moved = jax.random.randint(jax.random.fold_in(own_key, 1), (couples,), 0, 1 << 20) % (slack + 1)
    sizes = sizes.at[1:1 + 2 * couples:2].set(giver - moved).at[2:2 + 2 * couples:2].set(sink + moved)
    return sizes[jax.random.permutation(jax.random.fold_in(own_key, 2), amount)]


def normal_values(own_key, dims, deviation, bound, shards=(), kind=jnp.bfloat16):
    values = jax.random.normal(own_key, dims, jnp.float32) * deviation
    if len(shards) > 0:
        values = block_levels(own_key, dims, shards, -0.22, 0.18) * values
    return jnp.clip(values, min=-bound, max=bound).astype(kind)


def setup_inputs(seed: int = 0) -> dict:
    streams_of = jax.random.split(jax.random.key(seed), 10)
    query = normal_values(streams_of[0], (COMP_TOK, HQ * HD), 1.0, 6.0, ((0, 768),))
    comp_key = normal_values(streams_of[1], (COMP_TOK, HK * HD), 1.0, 6.0, ((0, 768),))
    comp_value = normal_values(streams_of[2], (COMP_TOK, HK * HD), 1.0, 6.0, ((0, 768),))
    prompt_key = normal_values(streams_of[3], (PROMPT_TOK, HK * HD), 1.0, 6.0, ((0, 768),))
    prompt_value = normal_values(streams_of[4], (PROMPT_TOK, HK * HD), 1.0, 6.0, ((0, 768),))
    d_out = normal_values(streams_of[5], (COMP_TOK, HQ * HD), 1.0, 6.0, ((0, 768),))
    q_gain = jnp.clip(1.0 + 0.1 * jax.random.normal(streams_of[6], (HD,), jnp.float32), 0.5, 1.5)
    k_gain = jnp.clip(1.0 + 0.1 * jax.random.normal(streams_of[7], (HD,), jnp.float32), 0.5, 1.5)
    lengths = ragged_sizes(streams_of[8], SAMPLES, SAMPLES * C_DEV * 5 // 8, C_DEV, 2).astype(jnp.int32)
    return {"query": query, "comp_key": comp_key, "comp_value": comp_value, "prompt_key": prompt_key, "prompt_value": prompt_value, "d_out": d_out, "q_gain": q_gain, "k_gain": k_gain, "lengths": lengths}


EPS = 1e-06

def widen(value):
    return lax.optimization_barrier(value).astype(jnp.float32)

def normalize(vectors, gain):
    wide = vectors.astype(jnp.float32)
    inverse = lax.rsqrt(lax.optimization_barrier(jnp.mean(wide * wide, axis=-1, keepdims=True)) + EPS)
    unit = wide * inverse
    return ((unit * gain).astype(jnp.bfloat16), unit, inverse)

def norm_back(grad, unit, inverse, gain):
    scaled = grad * gain
    back = inverse * (scaled - unit * lax.optimization_barrier(jnp.mean(scaled * unit, axis=-1, keepdims=True)))
    return (back, lax.optimization_barrier(jnp.sum((grad * unit).reshape(-1, unit.shape[-1]), axis=0)))

def attend_back(normed_query, keys, values, grad_out, visible):
    count = normed_query.shape[0]
    groups = HQ // HK
    scale = HD ** (-0.5)
    query_four = widen(normed_query).reshape(count, HK, groups, HD)
    keys_wide = widen(keys)
    values_wide = values.astype(jnp.float32)
    grad_four = grad_out.astype(jnp.float32).reshape(count, HK, groups, HD)
    scores = jnp.einsum('chgd,khd->hgck', query_four, keys_wide) * scale
    expo = jnp.where(visible, jnp.exp(scores), 0.0)
    probs = expo / lax.optimization_barrier(jnp.sum(expo, axis=-1, keepdims=True))
    rounded = widen(probs.astype(jnp.bfloat16))
    output = jnp.einsum('hgck,khd->chgd', rounded, values_wide)
    delta = jnp.transpose(lax.optimization_barrier(jnp.sum(grad_four * output, axis=-1)), (1, 2, 0))[..., None]
    dprob = jnp.einsum('chgd,khd->hgck', grad_four, values_wide)
    dscore = widen((probs * (dprob - delta)).astype(jnp.bfloat16))
    dquery = (jnp.einsum('hgck,khd->chgd', dscore, keys_wide) * scale).reshape(count, HQ, HD)
    dkey = jnp.einsum('hgck,chgd->khd', dscore, query_four) * scale
    dvalue = jnp.einsum('hgck,chgd->khd', rounded, grad_four)
    return (dquery, dkey, dvalue)

def reference(query, comp_key, comp_value, prompt_key, prompt_value, d_out, q_gain, k_gain, lengths):
    count = C_DEV
    width_q = HQ * HD
    width_k = HK * HD
    rows = jnp.arange(count, dtype=jnp.int32)
    visible = jnp.concatenate([jnp.ones((count, PROMPT), bool), rows[None, :] <= rows[:, None]], axis=1)

    def one_prompt(items):
        pkey, pvalue, queries, ckeys, cvalues, grads, lens = items
        pnorm, punit, pinv = normalize(pkey.reshape(PROMPT, HK, HD), k_gain)
        pvals = pvalue.reshape(PROMPT, HK, HD)

        def one_sample(carry, sample):
            key_acc, value_acc, gain_query, gain_key = carry
            qrow, krow, vrow, grow, length = sample
            qnorm, qunit, qinv = normalize(qrow.reshape(count, HQ, HD), q_gain)
            cnorm, cunit, cinv = normalize(krow.reshape(count, HK, HD), k_gain)
            live = (rows < length)[:, None]
            masked = jnp.where(live, grow, jnp.zeros_like(grow))
            keys = jnp.concatenate([pnorm, cnorm], axis=0)
            values = jnp.concatenate([pvals, vrow.reshape(count, HK, HD)], axis=0)
            dquery, dkey, dvalue = attend_back(qnorm, keys, values, masked.reshape(count, HQ, HD), visible)
            dq, gq = norm_back(dquery, qunit, qinv, q_gain)
            dck, gk = norm_back(dkey[PROMPT:], cunit, cinv, k_gain)
            carry = (key_acc + dkey[:PROMPT], value_acc + dvalue[:PROMPT], gain_query + gq, gain_key + gk)
            emitted = (dq.reshape(count, width_q).astype(jnp.bfloat16), dck.reshape(count, width_k).astype(jnp.bfloat16), dvalue[PROMPT:].reshape(count, width_k).astype(jnp.bfloat16))
            return (carry, emitted)
        zeros = jnp.zeros((PROMPT, HK, HD), jnp.float32)
        start = (zeros, zeros, jnp.zeros((HD,), jnp.float32), jnp.zeros((HD,), jnp.float32))
        final, emitted = lax.scan(one_sample, start, (queries, ckeys, cvalues, grads, lens))
        key_acc, value_acc, gain_query, gain_key = final
        dpk, gkp = norm_back(key_acc, punit, pinv, k_gain)
        return (emitted[0], emitted[1], emitted[2], dpk.reshape(PROMPT, width_k).astype(jnp.bfloat16), value_acc.reshape(PROMPT, width_k).astype(jnp.bfloat16), gain_query, gain_key + gkp)
    items = (prompt_key.reshape(N_DP, PROMPT, width_k), prompt_value.reshape(N_DP, PROMPT, width_k), query.reshape(N_DP, N_GROUP, count, width_q), comp_key.reshape(N_DP, N_GROUP, count, width_k), comp_value.reshape(N_DP, N_GROUP, count, width_k), d_out.reshape(N_DP, N_GROUP, count, width_q), lengths.reshape(N_DP, N_GROUP))
    results = lax.map(one_prompt, items)
    d_query = results[0].reshape(COMP_TOK, width_q)
    d_comp_key = results[1].reshape(COMP_TOK, width_k)
    d_comp_value = results[2].reshape(COMP_TOK, width_k)
    d_prompt_key = results[3].reshape(PROMPT_TOK, width_k)
    d_prompt_value = results[4].reshape(PROMPT_TOK, width_k)
    return (d_query, d_comp_key, d_comp_value, d_prompt_key, d_prompt_value, lax.optimization_barrier(jnp.sum(results[5], axis=0)), lax.optimization_barrier(jnp.sum(results[6], axis=0)))
```

```python
import functools

import jax
import jax.numpy as jnp
from jax import lax
from jax.experimental import pallas as pl
from jax.experimental.pallas import tpu as pltpu
from jax.sharding import Mesh
from jax.sharding import PartitionSpec as P

HD = 128
HQ = 32
HK = 4
PER = HQ // HK
TOK = 128
SHARD = 4
PEERS = 32
REPLICAS = 24
EPS = 1e-06
SCALE = HD ** (-0.5)
LOG2E = 1.4426950408889634
GROUP = ("group_0", "group_1", "group_2")
DP = ("dp_0", "dp_1")
DP_GROUP = ("dp_0", "dp_1", "group_0", "group_1", "group_2")
NT = (((1,), (1,)), ((), ()))
TN = (((0,), (0,)), ((), ()))
NN = (((1,), (0,)), ((), ()))


def dot(a, b, dims):
    return lax.dot_general(a, b, dims, preferred_element_type=jnp.float32)


def unit_of(x):
    wide = x.astype(jnp.float32)
    inverse = lax.rsqrt(jnp.mean(wide * wide, axis=-1, keepdims=True) + EPS)
    return wide * inverse, inverse


def back_of(grad, unit, inverse, gain):
    scaled = grad * gain
    return inverse * (scaled - unit * jnp.mean(scaled * unit, axis=-1, keepdims=True))


def rows_eight(x):
    return jnp.sum(x.reshape(x.shape[0] // 8, 8, x.shape[1]), axis=0)


def unmix(mixed):
    pairs = mixed.reshape(PEERS // 2, 2, 8, HD)
    even, odd = pairs[:, 0], pairs[:, 1]
    low = lax.broadcasted_iota(jnp.int32, even.shape, 1) < SHARD
    first = jnp.where(low, even, pltpu.roll(odd, SHARD, 1))
    second = jnp.where(low, pltpu.roll(even, SHARD, 1), odd)
    return first.reshape(TOK, HD), second.reshape(TOK, HD)


def mix(first, second):
    one = first.reshape(PEERS // 2, 8, HD)
    two = second.reshape(PEERS // 2, 8, HD)
    low = lax.broadcasted_iota(jnp.int32, one.shape, 1) < SHARD
    even = jnp.where(low, one, pltpu.roll(two, SHARD, 1))
    odd = jnp.where(low, pltpu.roll(one, SHARD, 1), two)
    return jnp.stack([even, odd], axis=1).reshape(PEERS, 8, HD)


def pieces(x):
    high = x.astype(jnp.bfloat16).astype(jnp.float32)
    middle = (x - high).astype(jnp.bfloat16).astype(jnp.float32)
    return [high, middle, x - high - middle]


def attention_kernel(
    len_ref, q_ref, do_ref, ck_ref, cv_ref, pkv_ref, qg_ref, kg_ref,
    dq_ref, dck_ref, dcv_ref, term_ref,
    qn_s, g_s, p_s, ds_s, acc_s,
):
    step = pl.program_id(0)
    qg = qg_ref[...]
    kg = kg_ref[...]

    @pl.when(step == 0)
    def _():
        acc_s[...] = jnp.zeros_like(acc_s)

    pk, pv = unmix(pkv_ref[...].astype(jnp.float32))
    kraw = jnp.concatenate([pk, ck_ref[...].astype(jnp.float32)], axis=0)
    kunit, kinv = unit_of(kraw)
    kn = (kunit * kg).astype(jnp.bfloat16)
    v = jnp.concatenate([pv.astype(jnp.bfloat16), cv_ref[...]], axis=0)

    live = lax.broadcasted_iota(jnp.int32, (TOK, HD), 0) < len_ref[0]
    for j in range(PER):
        cols, rows = pl.ds(j * HD, HD), pl.ds(j * TOK, TOK)
        qunit, _ = unit_of(q_ref[:, cols])
        qn_s[rows, :] = (qunit * qg).astype(jnp.bfloat16)
        g_s[rows, :] = jnp.where(live, do_ref[:, cols].astype(jnp.float32), 0.0).astype(jnp.bfloat16)

    key = lax.broadcasted_iota(jnp.int32, (TOK, 2 * TOK), 0)
    slot = lax.rem(lax.broadcasted_iota(jnp.int32, (TOK, 2 * TOK), 1), TOK)
    seen = key <= slot
    qacc = jnp.zeros((8, HD), jnp.float32)
    for pair in range(PER // 2):
        span = pl.ds(pair * 2 * TOK, 2 * TOK)
        qn, g = qn_s[span, :], g_s[span, :]
        score = dot(kn, qn, NT) * (SCALE * LOG2E)
        dprob = dot(v, g, NT)
        expo = jnp.exp2(score)
        expo = jnp.concatenate([expo[:TOK], jnp.where(seen, expo[TOK:], 0.0)], axis=0)
        total = jnp.sum(expo, axis=0, keepdims=True)
        weighted = jnp.sum(expo * dprob, axis=0, keepdims=True)
        inv = 1.0 / total
        prob = expo * inv
        dscore = (prob * (dprob - weighted * inv)).astype(jnp.bfloat16)
        p_s[:, span] = prob.astype(jnp.bfloat16)
        ds_s[:, span] = dscore
        dn = dot(dscore, kn, TN) * SCALE
        for half in range(2):
            cols = pl.ds((pair * 2 + half) * HD, HD)
            unit, inverse = unit_of(q_ref[:, cols])
            grad = dn[half * TOK : (half + 1) * TOK]
            dq_ref[:, cols] = back_of(grad, unit, inverse, qg).astype(jnp.bfloat16)
            qacc += rows_eight(grad * unit)

    dv = dot(p_s[...], g_s[...], NN)
    dk = dot(ds_s[...], qn_s[...], NN) * SCALE
    dck_ref[...] = back_of(dk[TOK:], kunit[TOK:], kinv[TOK:], kg).astype(jnp.bfloat16)
    dcv_ref[...] = dv[TOK:].astype(jnp.bfloat16)
    here = pl.ds(pl.multiple_of(step * HD, HD), HD)
    term_ref[:, :, here] = mix(dk[:TOK], dv[:TOK]).astype(jnp.bfloat16)
    acc_s[0:8, :] += qacc
    acc_s[8:16, :] += rows_eight(dk * kunit)

    @pl.when(step == HK - 1)
    def _():
        rows = pieces(jnp.sum(acc_s[0:8, :], axis=0, keepdims=True))
        rows += pieces(jnp.sum(acc_s[8:16, :], axis=0, keepdims=True))
        rows += [jnp.zeros((2, HD), jnp.float32)]
        tile = jnp.broadcast_to(jnp.concatenate(rows, axis=0)[None], (PEERS, 8, HD))
        term_ref[:, :, HK * HD :] = tile.astype(jnp.bfloat16)


def attention(lengths, query, d_out, comp_key, comp_value, prompt, q_gain, k_gain):
    wide = pl.BlockSpec((TOK, PER * HD), lambda h, *_: (0, h))
    narrow = pl.BlockSpec((TOK, HD), lambda h, *_: (0, h))
    mixed = pl.BlockSpec((PEERS, 8, HD), lambda h, *_: (0, 0, h))
    gain = pl.BlockSpec((1, HD), lambda h, *_: (0, 0))
    whole = pl.BlockSpec((PEERS, 8, (HK + 1) * HD), lambda h, *_: (0, 0, 0))
    return pl.pallas_call(
        attention_kernel,
        grid_spec=pltpu.PrefetchScalarGridSpec(
            num_scalar_prefetch=1,
            grid=(HK,),
            in_specs=[wide, wide, narrow, narrow, mixed, gain, gain],
            out_specs=[wide, narrow, narrow, whole],
            scratch_shapes=[
                pltpu.VMEM((PER * TOK, HD), jnp.bfloat16),
                pltpu.VMEM((PER * TOK, HD), jnp.bfloat16),
                pltpu.VMEM((2 * TOK, PER * TOK), jnp.bfloat16),
                pltpu.VMEM((2 * TOK, PER * TOK), jnp.bfloat16),
                pltpu.VMEM((16, HD), jnp.float32),
            ],
        ),
        out_shape=[
            jax.ShapeDtypeStruct((TOK, HQ * HD), jnp.bfloat16),
            jax.ShapeDtypeStruct((TOK, HK * HD), jnp.bfloat16),
            jax.ShapeDtypeStruct((TOK, HK * HD), jnp.bfloat16),
            jax.ShapeDtypeStruct((PEERS, 8, (HK + 1) * HD), jnp.bfloat16),
        ],
        cost_estimate=pl.CostEstimate(
            flops=5 * 2 * HQ * TOK * 2 * TOK * HD, bytes_accessed=5 << 20, transcendentals=HQ * TOK * 2 * TOK
        ),
        compiler_params=pltpu.CompilerParams(dimension_semantics=("arbitrary",)),
        name="attention_back",
    )(lengths, query, d_out, comp_key, comp_value, prompt, q_gain.reshape(1, HD), k_gain.reshape(1, HD))


def pack_kernel(key_ref, value_ref, out_ref):
    own = jnp.concatenate([key_ref[...].astype(jnp.float32), value_ref[...].astype(jnp.float32)], axis=0)
    out_ref[...] = jnp.broadcast_to(own.astype(jnp.bfloat16)[None], out_ref.shape)


def pack(prompt_key, prompt_value):
    return pl.pallas_call(
        pack_kernel,
        out_shape=jax.ShapeDtypeStruct((PEERS, 8, HK * HD), jnp.bfloat16),
        name="prompt_pack",
    )(prompt_key, prompt_value)


def finish_kernel(arrived_ref, key_ref, kg_ref, dk_ref, dv_ref, gain_ref):
    both = jnp.sum(arrived_ref[...].astype(jnp.float32), axis=0)
    tail = both[:, HK * HD :]
    for row in range(2):
        total = tail[3 * row : 3 * row + 1] + (tail[3 * row + 1 : 3 * row + 2] + tail[3 * row + 2 : 3 * row + 3])
        gain_ref[:, row : row + 1, :] = jnp.broadcast_to(total[None], (REPLICAS, 1, HD))
    for h in range(HK):
        cols = pl.ds(h * HD, HD)
        unit, inverse = unit_of(key_ref[:, cols])
        grad = both[:SHARD, h * HD : (h + 1) * HD]
        dk_ref[:, cols] = back_of(grad, unit, inverse, kg_ref[...]).astype(jnp.bfloat16)
    dv_ref[...] = both[SHARD:, : HK * HD].astype(jnp.bfloat16)


def finish(arrived, prompt_key, k_gain):
    out = jax.ShapeDtypeStruct((SHARD, HK * HD), jnp.bfloat16)
    gains = jax.ShapeDtypeStruct((REPLICAS, 2, HD), jnp.float32)
    return pl.pallas_call(finish_kernel, out_shape=[out, out, gains], name="prompt_back")(
        arrived, prompt_key, k_gain.reshape(1, HD)
    )


def exchange(x, axes):
    return lax.all_to_all(x, axes, split_axis=0, concat_axis=0, tiled=True)


def local(query, comp_key, comp_value, prompt_key, prompt_value, d_out, q_gain, k_gain, lengths):
    prompt = exchange(pack(prompt_key, prompt_value), GROUP)
    dq, dck, dcv, term = attention(
        lengths, query, d_out, comp_key, comp_value, prompt, q_gain, k_gain
    )
    dpk, dpv, gains = finish(exchange(term, GROUP), prompt_key, k_gain)
    gains = jnp.sum(exchange(gains, DP), axis=0)
    return (dq, dck, dcv, dpk, dpv, gains[0], gains[1])


def solution(mesh):
    finer = Mesh(
        mesh.devices.reshape(12, 2, 4, 4, 2), ("dp_0", "dp_1", "group_0", "group_1", "group_2")
    )
    rows = P(DP_GROUP, None)
    return jax.shard_map(
        local,
        mesh=finer,
        in_specs=(rows, rows, rows, rows, rows, rows, P(), P(), P(DP_GROUP)),
        out_specs=(rows, rows, rows, rows, rows, P(), P()),
        check_vma=False,
    )
```

```python
import functools

import jax
import jax.numpy as jnp
from jax import lax
from jax.experimental import pallas as pl
from jax.experimental.pallas import tpu as pltpu
from jax.sharding import Mesh
from jax.sharding import PartitionSpec as P

HD = 128
HQ = 32
HK = 4
PER = HQ // HK
TOK = 128
SHARD = 4
PEERS = 32
PLACES = PEERS // 2
REPLICAS = 48
EPS = 1e-06
SCALE = HD ** (-0.5)
LOG2E = 1.4426950408889634
GROUP = ("group_0", "group_1", "group_2")
CORE = "group_2"
PLACE = ("group_0", "group_1")
DP_CORE = ("dp_0", "dp_1", "group_2")
DP_GROUP = ("dp_0", "dp_1", "group_0", "group_1", "group_2")
NT = (((1,), (1,)), ((), ()))
TN = (((0,), (0,)), ((), ()))
NN = (((1,), (0,)), ((), ()))


def dot(a, b, dims):
    return lax.dot_general(a, b, dims, preferred_element_type=jnp.float32)


def unit_of(x):
    wide = x.astype(jnp.float32)
    inverse = lax.rsqrt(jnp.mean(wide * wide, axis=-1, keepdims=True) + EPS)
    return wide * inverse, inverse


def back_of(grad, unit, inverse, gain):
    scaled = grad * gain
    return inverse * (scaled - unit * jnp.mean(scaled * unit, axis=-1, keepdims=True))


def rows_eight(x):
    return jnp.sum(x.reshape(x.shape[0] // 8, 8, x.shape[1]), axis=0)


def unmix(mixed):
    pairs = mixed.reshape(PEERS // 2, 2, 8, HD)
    even, odd = pairs[:, 0], pairs[:, 1]
    low = lax.broadcasted_iota(jnp.int32, even.shape, 1) < SHARD
    first = jnp.where(low, even, pltpu.roll(odd, SHARD, 1))
    second = jnp.where(low, pltpu.roll(even, SHARD, 1), odd)
    return first.reshape(TOK, HD), second.reshape(TOK, HD)


def mix(first, second):
    one = first.reshape(PEERS // 2, 8, HD)
    two = second.reshape(PEERS // 2, 8, HD)
    low = lax.broadcasted_iota(jnp.int32, one.shape, 1) < SHARD
    even = jnp.where(low, one, pltpu.roll(two, SHARD, 1))
    odd = jnp.where(low, pltpu.roll(one, SHARD, 1), two)
    return even, odd


def pieces(x):
    high = x.astype(jnp.bfloat16).astype(jnp.float32)
    middle = (x - high).astype(jnp.bfloat16).astype(jnp.float32)
    return [high, middle, x - high - middle]


def params(mib, *semantics):
    return pltpu.CompilerParams(vmem_limit_bytes=int(mib * 2**20), dimension_semantics=semantics or None)


def pack_kernel(key_ref, value_ref, out_ref):
    own = jnp.concatenate([key_ref[...].astype(jnp.float32), value_ref[...].astype(jnp.float32)], axis=0)
    out_ref[...] = jnp.broadcast_to(own.astype(jnp.bfloat16)[None], out_ref.shape)


def pack(prompt_key, prompt_value):
    return pl.pallas_call(
        pack_kernel,
        out_shape=jax.ShapeDtypeStruct((PEERS, 8, HK * HD), jnp.bfloat16),
        compiler_params=params(4),
        name="prompt_pack",
    )(prompt_key, prompt_value)


def own_kernel(len_ref, q_ref, do_ref, ck_ref, cv_ref, qg_ref, kg_ref, qn_ref, g_ref, e_ref, dp_ref, sums_ref):
    live = lax.broadcasted_iota(jnp.int32, (TOK, HD), 0) < len_ref[0]
    kunit, _ = unit_of(ck_ref[...])
    kn = (kunit * kg_ref[...]).astype(jnp.bfloat16)
    v = cv_ref[...]
    key = lax.broadcasted_iota(jnp.int32, (TOK, 2 * TOK), 0)
    slot = lax.rem(lax.broadcasted_iota(jnp.int32, (TOK, 2 * TOK), 1), TOK)
    seen = key <= slot
    for pair in range(PER // 2):
        span = pl.ds(pair * 2 * TOK, 2 * TOK)
        for j in (2 * pair, 2 * pair + 1):
            cols, rows = pl.ds(j * HD, HD), pl.ds(j * TOK, TOK)
            qunit, _ = unit_of(q_ref[:, cols])
            qn_ref[rows, :] = (qunit * qg_ref[...]).astype(jnp.bfloat16)
            g_ref[rows, :] = jnp.where(live, do_ref[:, cols].astype(jnp.float32), 0.0).astype(jnp.bfloat16)
        expo = jnp.exp2(dot(kn, qn_ref[span, :], NT) * (SCALE * LOG2E))
        expo = jnp.where(seen, expo, 0.0)
        dprob = dot(v, g_ref[span, :], NT)
        e_ref[0, :, span] = expo.astype(jnp.bfloat16)
        dp_ref[0, :, span] = dprob.astype(jnp.bfloat16)
        sums_ref[0, 0:1, span] = jnp.sum(expo, axis=0, keepdims=True)
        sums_ref[0, 1:2, span] = jnp.sum(expo * dprob, axis=0, keepdims=True)


QUERIES = PER * TOK
WIDE = pl.BlockSpec((TOK, PER * HD), lambda h, *_: (0, h))
NARROW = pl.BlockSpec((TOK, HD), lambda h, *_: (0, h))
MIXED = pl.BlockSpec((PEERS, 8, HD), lambda h, *_: (0, 0, h))
GAIN = pl.BlockSpec((1, HD), lambda h, *_: (0, 0))
STACK = pl.BlockSpec((QUERIES, HD), lambda h, *_: (h, 0))


def per_head(rows, columns):
    return pl.BlockSpec((1, rows, columns), lambda h, *_: (h, 0, 0))


def own(lengths, query, d_out, comp_key, comp_value, q_gain, k_gain):
    return pl.pallas_call(
        own_kernel,
        grid_spec=pltpu.PrefetchScalarGridSpec(
            num_scalar_prefetch=1,
            grid=(HK,),
            in_specs=[WIDE, WIDE, NARROW, NARROW, GAIN, GAIN],
            out_specs=[STACK, STACK, per_head(TOK, QUERIES), per_head(TOK, QUERIES), per_head(2, QUERIES)],
        ),
        out_shape=[
            jax.ShapeDtypeStruct((HQ * TOK, HD), jnp.bfloat16),
            jax.ShapeDtypeStruct((HQ * TOK, HD), jnp.bfloat16),
            jax.ShapeDtypeStruct((HK, TOK, QUERIES), jnp.bfloat16),
            jax.ShapeDtypeStruct((HK, TOK, QUERIES), jnp.bfloat16),
            jax.ShapeDtypeStruct((HK, 2, QUERIES), jnp.float32),
        ],
        cost_estimate=pl.CostEstimate(
            flops=2 * 2 * HQ * TOK * TOK * HD, bytes_accessed=8 << 20, transcendentals=HQ * TOK * TOK
        ),
        compiler_params=params(24, "arbitrary"),
        name="own_scores",
    )(lengths, query, d_out, comp_key, comp_value, q_gain, k_gain)


def all_keys(pk, ck, kg_ref):
    raw = jnp.concatenate([pk, ck.astype(jnp.float32)], axis=0)
    unit, inverse = unit_of(raw)
    return unit, inverse, (unit * kg_ref[...]).astype(jnp.bfloat16)


def score_kernel(
    core_ref, qn_hbm, g_hbm, e_hbm, d_hbm, sums_hbm, ck_hbm, pkv_hbm, qg_ref, kg_ref,
    ds_hbm, dck_ref, dcv_ref, keep_ref, send_ref, gain_ref,
    sums_ref, ck_ref, pkv_ref, qn_s, g_s, e_s, d_s, p_s, ds_s, acc_s, all_sem, in_sem, out_sem,
):
    pairs = ((pkv_hbm, pkv_ref), (ck_hbm, ck_ref), (sums_hbm, sums_ref))
    common = [pltpu.make_async_copy(s, t, all_sem.at[n]) for n, (s, t) in enumerate(pairs)]
    for copy in common:
        copy.start()
    def loads(h):
        rows = pl.ds(pl.multiple_of(h * QUERIES, QUERIES), QUERIES)
        sources = (qn_hbm.at[rows], g_hbm.at[rows], e_hbm.at[h], d_hbm.at[h])
        targets = (qn_s.at[h], g_s.at[h], e_s.at[h], d_s.at[h])
        return [pltpu.make_async_copy(s, t, in_sem.at[h, n]) for n, (s, t) in enumerate(zip(sources, targets))]

    def store(h):
        return pltpu.make_async_copy(ds_s.at[h], ds_hbm.at[h], out_sem.at[h])

    for h in range(HK):
        for copy in loads(h):
            copy.start()
    first_core = core_ref[0] == 0
    acc_s[...] = jnp.zeros_like(acc_s)
    for copy in common:
        copy.wait()

    def head(h, carry):
        cols = pl.ds(pl.multiple_of(h * HD, HD), HD)
        pk, pv = unmix(pkv_ref[:, :, cols].astype(jnp.float32))
        unit, inverse, kn = all_keys(pk, ck_ref[:, cols], kg_ref)
        v = pv.astype(jnp.bfloat16)
        for copy in loads(h):
            copy.wait()
        for pair in range(PER // 2):
            span = pl.ds(pair * 2 * TOK, 2 * TOK)
            expo = jnp.exp2(dot(kn[:TOK], qn_s[h, span, :], NT) * (SCALE * LOG2E))
            dprob = dot(v, g_s[h, span, :], NT)
            inv = 1.0 / (sums_ref[h, 0:1, span] + jnp.sum(expo, axis=0, keepdims=True))
            delta = (sums_ref[h, 1:2, span] + jnp.sum(expo * dprob, axis=0, keepdims=True)) * inv
            for half in range(2):
                rows = pl.ds(half * TOK, TOK)
                e = e_s[h, :, span].astype(jnp.float32) if half else expo
                d = d_s[h, :, span].astype(jnp.float32) if half else dprob
                prob = e * inv
                p_s[rows, span] = prob.astype(jnp.bfloat16)
                ds_s[h, rows, span] = (prob * (d - delta)).astype(jnp.bfloat16)
        ds_s[h, :, QUERIES:] = kn
        store(h).start()
        dk = dot(ds_s[h, :, :QUERIES], qn_s[h], NN) * SCALE
        dv = dot(p_s[...], g_s[h], NN)
        acc_s[0:8, :] += rows_eight(dk * kn.astype(jnp.float32))
        acc_s[8:16, :] += rows_eight(dk * unit)
        dck_ref[:, cols] = back_of(dk[TOK:], unit[TOK:], inverse[TOK:], kg_ref[...]).astype(jnp.bfloat16)
        dcv_ref[:, cols] = dv[TOK:].astype(jnp.bfloat16)
        zero, one = mix(dk[:TOK], dv[:TOK])
        keep_ref[:, :, cols] = jnp.where(first_core, zero, one).astype(jnp.bfloat16)
        send_ref[:, :, cols] = jnp.where(first_core, one, zero).astype(jnp.bfloat16)
        return carry

    for h in range(HK):
        head(h, 0)
    rows = [jnp.sum(acc_s[0:8, :], axis=0, keepdims=True) / qg_ref[...]]
    rows += [jnp.sum(acc_s[8:16, :], axis=0, keepdims=True)]
    gain_ref[...] = jnp.broadcast_to(jnp.concatenate(rows, axis=0)[None], gain_ref.shape)
    for h in range(HK):
        store(h).wait()


VMEM = pl.BlockSpec(memory_space=pltpu.VMEM)
ANY = pl.BlockSpec(memory_space=pl.ANY)


def scores(core, qn, g, e, dp, sums, comp_key, prompt, q_gain, k_gain):
    half = jax.ShapeDtypeStruct((PLACES, 8, HK * HD), jnp.bfloat16)
    return pl.pallas_call(
        score_kernel,
        in_specs=[pl.BlockSpec(memory_space=pltpu.SMEM)] + [ANY] * 7 + [VMEM] * 2,
        out_specs=[ANY] + [VMEM] * 5,
        out_shape=[
            jax.ShapeDtypeStruct((HK, 2 * TOK, QUERIES + HD), jnp.bfloat16),
            jax.ShapeDtypeStruct((TOK, HK * HD), jnp.bfloat16),
            jax.ShapeDtypeStruct((TOK, HK * HD), jnp.bfloat16),
            half,
            half,
            jax.ShapeDtypeStruct((REPLICAS, 2, HD), jnp.float32),
        ],
        scratch_shapes=[
            pltpu.VMEM((HK, 2, QUERIES), jnp.float32),
            pltpu.VMEM((TOK, HK * HD), jnp.bfloat16),
            pltpu.VMEM((PEERS, 8, HK * HD), jnp.bfloat16),
            pltpu.VMEM((HK, QUERIES, HD), jnp.bfloat16),
            pltpu.VMEM((HK, QUERIES, HD), jnp.bfloat16),
            pltpu.VMEM((HK, TOK, QUERIES), jnp.bfloat16),
            pltpu.VMEM((HK, TOK, QUERIES), jnp.bfloat16),
            pltpu.VMEM((2 * TOK, QUERIES), jnp.bfloat16),
            pltpu.VMEM((HK, 2 * TOK, QUERIES + HD), jnp.bfloat16),
            pltpu.VMEM((16, HD), jnp.float32),
            pltpu.SemaphoreType.DMA((3,)),
            pltpu.SemaphoreType.DMA((HK, 4)),
            pltpu.SemaphoreType.DMA((HK,)),
        ],
        cost_estimate=pl.CostEstimate(
            flops=6 * 2 * HQ * TOK * TOK * HD, bytes_accessed=7 << 20, transcendentals=HQ * TOK * TOK
        ),
        compiler_params=params(50.75),
        name="all_scores",
    )(core, qn, g, e, dp, sums, comp_key, prompt, q_gain, k_gain)


def query_kernel(ds_ref, q_ref, qg_ref, dq_ref):
    kn = ds_ref[0, :, QUERIES:]
    for pair in range(PER // 2):
        dn = dot(ds_ref[0, :, pair * 2 * TOK : (pair + 1) * 2 * TOK], kn, TN) * SCALE
        for half in range(2):
            cols = pl.ds((pair * 2 + half) * HD, HD)
            unit, inverse = unit_of(q_ref[:, cols])
            grad = dn[half * TOK : (half + 1) * TOK]
            dq_ref[:, cols] = back_of(grad, unit, inverse, qg_ref[...]).astype(jnp.bfloat16)


def queries_back(ds, query, q_gain):
    return pl.pallas_call(
        query_kernel,
        grid=(HK,),
        in_specs=[per_head(2 * TOK, QUERIES + HD), WIDE, GAIN],
        out_specs=WIDE,
        out_shape=jax.ShapeDtypeStruct((TOK, HQ * HD), jnp.bfloat16),
        cost_estimate=pl.CostEstimate(
            flops=2 * 2 * HQ * TOK * TOK * HD, bytes_accessed=5 << 20, transcendentals=0
        ),
        compiler_params=params(60, "arbitrary"),
        name="query_back",
    )(ds, query, q_gain)


def join_kernel(keep_ref, got_ref, out_ref):
    total = keep_ref[...].astype(jnp.float32) + got_ref[...].astype(jnp.float32)
    out_ref[:, :, : HK * HD] = total.astype(jnp.bfloat16)


def join(keep, got):
    return pl.pallas_call(
        join_kernel,
        out_shape=jax.ShapeDtypeStruct((PLACES, 8, (HK + 1) * HD), jnp.bfloat16),
        cost_estimate=pl.CostEstimate(flops=1 << 17, bytes_accessed=400 << 10, transcendentals=0),
        compiler_params=params(4),
        name="core_join",
    )(keep, got)


def relay_kernel(arrived_ref, joined_hbm, out_ref):
    both = jnp.sum(arrived_ref[...], axis=0)
    rows = pieces(both[0:1]) + pieces(both[1:2]) + [jnp.zeros((2, HD), jnp.float32)]
    tile = jnp.concatenate(rows, axis=0)[None]
    out_ref[...] = jnp.broadcast_to(tile, out_ref.shape).astype(jnp.bfloat16)


def relay(arrived, joined):
    return pl.pallas_call(
        relay_kernel,
        grid=(1,),
        in_specs=[pl.BlockSpec((REPLICAS, 2, HD), lambda i: (0, 0, 0)), ANY],
        out_specs=pl.BlockSpec((PLACES, 8, HD), lambda i: (0, 0, HK)),
        out_shape=jax.ShapeDtypeStruct(joined.shape, joined.dtype),
        input_output_aliases={1: 0},
        compiler_params=params(4),
        name="gain_relay",
    )(arrived, joined)


def finish_kernel(arrived_ref, key_ref, kg_ref, dk_ref, dv_ref, gq_ref, gk_ref):
    both = jnp.sum(arrived_ref[...].astype(jnp.float32), axis=0)
    for row, ref in ((0, gq_ref), (3, gk_ref)):
        high, middle, low = [both[row + n : row + n + 1, HK * HD :] for n in range(3)]
        ref[...] = high + (middle + low)
    for h in range(HK):
        cols = pl.ds(h * HD, HD)
        unit, inverse = unit_of(key_ref[:, cols])
        grad = both[:SHARD, h * HD : (h + 1) * HD]
        dk_ref[:, cols] = back_of(grad, unit, inverse, kg_ref[...]).astype(jnp.bfloat16)
    dv_ref[...] = both[SHARD:, : HK * HD].astype(jnp.bfloat16)


def finish(arrived, prompt_key, k_gain):
    out = jax.ShapeDtypeStruct((SHARD, HK * HD), jnp.bfloat16)
    gain = jax.ShapeDtypeStruct((1, HD), jnp.float32)
    return pl.pallas_call(
        finish_kernel,
        out_shape=[out, out, gain, gain],
        cost_estimate=pl.CostEstimate(flops=1 << 20, bytes_accessed=300 << 10, transcendentals=0),
        compiler_params=params(4),
        name="prompt_back",
    )(arrived, prompt_key, k_gain)


def exchange(x, axes):
    return lax.all_to_all(x, axes, split_axis=0, concat_axis=0, tiled=True)


def local(query, comp_key, comp_value, prompt_key, prompt_value, d_out, q_gain, k_gain, lengths):
    q_gain, k_gain = q_gain.reshape(1, HD), k_gain.reshape(1, HD)
    core = lax.axis_index(CORE).reshape(1)
    prompt = exchange(pack(prompt_key, prompt_value), GROUP)
    owned = own(lengths, query, d_out, comp_key, comp_value, q_gain, k_gain)
    ds, dck, dcv, keep, send, gains = scores(core, *owned, comp_key, prompt, q_gain, k_gain)
    gains = exchange(gains, DP_CORE)
    joined = join(keep, lax.ppermute(send, CORE, [(0, 1), (1, 0)]))
    dq = queries_back(ds, query, q_gain)
    dpk, dpv, gain_q, gain_k = finish(exchange(relay(gains, joined), PLACE), prompt_key, k_gain)
    return (dq, dck, dcv, dpk, dpv, gain_q.reshape(HD), gain_k.reshape(HD))


def solution(mesh):
    finer = Mesh(
        mesh.devices.reshape(12, 2, 4, 4, 2), ("dp_0", "dp_1", "group_0", "group_1", "group_2")
    )
    rows = P(DP_GROUP, None)
    return jax.shard_map(
        local,
        mesh=finer,
        in_specs=(rows, rows, rows, rows, rows, rows, P(), P(), P(DP_GROUP)),
        out_specs=(rows, rows, rows, rows, rows, P(), P()),
        check_vma=False,
    )
```

```python
import functools

import jax
import jax.numpy as jnp
from jax import lax
from jax.experimental import pallas as pl
from jax.experimental.pallas import tpu as pltpu
from jax.sharding import Mesh
from jax.sharding import PartitionSpec as P

HD = 128
HQ = 32
HK = 4
PER = HQ // HK
TOK = 128
SHARD = 4
PEERS = 32
PLACES = PEERS // 2
REPLICAS = 48
SCORE_MIB = 51
EPS = 1e-06
SCALE = HD ** (-0.5)
LOG2E = 1.4426950408889634
GROUP = ("group_0", "group_1", "group_2")
CORE = "group_2"
PLACE = ("group_0", "group_1")
DP_CORE = ("dp_0", "dp_1", "group_2")
DP_GROUP = ("dp_0", "dp_1", "group_0", "group_1", "group_2")
NT = (((1,), (1,)), ((), ()))
TN = (((0,), (0,)), ((), ()))
NN = (((1,), (0,)), ((), ()))


def dot(a, b, dims):
    return lax.dot_general(a, b, dims, preferred_element_type=jnp.float32)


def unit_of(x):
    wide = x.astype(jnp.float32)
    inverse = lax.rsqrt(jnp.mean(wide * wide, axis=-1, keepdims=True) + EPS)
    return wide * inverse, inverse


def back_of(grad, unit, inverse, gain):
    scaled = grad * gain
    return inverse * (scaled - unit * jnp.mean(scaled * unit, axis=-1, keepdims=True))


def rows_eight(x):
    return jnp.sum(x.reshape(x.shape[0] // 8, 8, x.shape[1]), axis=0)


def unmix(mixed):
    pairs = mixed.reshape(PEERS // 2, 2, 8, HD)
    even, odd = pairs[:, 0], pairs[:, 1]
    low = lax.broadcasted_iota(jnp.int32, even.shape, 1) < SHARD
    first = jnp.where(low, even, pltpu.roll(odd, SHARD, 1))
    second = jnp.where(low, pltpu.roll(even, SHARD, 1), odd)
    return first.reshape(TOK, HD), second.reshape(TOK, HD)


def mix(first, second):
    one = first.reshape(PEERS // 2, 8, HD)
    two = second.reshape(PEERS // 2, 8, HD)
    low = lax.broadcasted_iota(jnp.int32, one.shape, 1) < SHARD
    even = jnp.where(low, one, pltpu.roll(two, SHARD, 1))
    odd = jnp.where(low, pltpu.roll(one, SHARD, 1), two)
    return even, odd


def pieces(x):
    high = x.astype(jnp.bfloat16).astype(jnp.float32)
    middle = (x - high).astype(jnp.bfloat16).astype(jnp.float32)
    return [high, middle, x - high - middle]


def params(mib, *semantics):
    return pltpu.CompilerParams(vmem_limit_bytes=int(mib * 2**20), dimension_semantics=semantics or None)


def pack_kernel(key_ref, value_ref, out_ref):
    own = jnp.concatenate([key_ref[...].astype(jnp.float32), value_ref[...].astype(jnp.float32)], axis=0)
    out_ref[...] = jnp.broadcast_to(own.astype(jnp.bfloat16)[None], out_ref.shape)


def pack(prompt_key, prompt_value):
    return pl.pallas_call(
        pack_kernel,
        out_shape=jax.ShapeDtypeStruct((PEERS, 8, HK * HD), jnp.bfloat16),
        compiler_params=params(60),
        name="prompt_pack",
    )(prompt_key, prompt_value)


def own_kernel(len_ref, q_ref, do_ref, qg_ref, qn_ref, g_ref):
    live = lax.broadcasted_iota(jnp.int32, (TOK, HD), 0) < len_ref[0]
    for j in range(PER):
        cols, rows = pl.ds(j * HD, HD), pl.ds(j * TOK, TOK)
        qunit, _ = unit_of(q_ref[:, cols])
        qn_ref[rows, :] = (qunit * qg_ref[...]).astype(jnp.bfloat16)
        g_ref[rows, :] = jnp.where(live, do_ref[:, cols].astype(jnp.float32), 0.0).astype(jnp.bfloat16)


QUERIES = PER * TOK
WIDE = pl.BlockSpec((TOK, PER * HD), lambda h, *_: (0, h))
NARROW = pl.BlockSpec((TOK, HD), lambda h, *_: (0, h))
MIXED = pl.BlockSpec((PEERS, 8, HD), lambda h, *_: (0, 0, h))
GAIN = pl.BlockSpec((1, HD), lambda h, *_: (0, 0))
STACK = pl.BlockSpec((QUERIES, HD), lambda h, *_: (h, 0))


def per_head(rows, columns):
    return pl.BlockSpec((1, rows, columns), lambda h, *_: (h, 0, 0))


def own(lengths, query, d_out, q_gain):
    stacked = jax.ShapeDtypeStruct((HQ * TOK, HD), jnp.bfloat16)
    return pl.pallas_call(
        own_kernel,
        grid_spec=pltpu.PrefetchScalarGridSpec(
            num_scalar_prefetch=1,
            grid=(HK,),
            in_specs=[WIDE, WIDE, GAIN],
            out_specs=[STACK, STACK],
        ),
        out_shape=[stacked, stacked],
        cost_estimate=pl.CostEstimate(flops=1 << 24, bytes_accessed=4 << 20, transcendentals=HQ * TOK),
        compiler_params=params(24, "arbitrary"),
        name="own_norms",
    )(lengths, query, d_out, q_gain)


def all_keys(pk, ck, kg_ref):
    raw = jnp.concatenate([pk, ck.astype(jnp.float32)], axis=0)
    unit, inverse = unit_of(raw)
    return unit, inverse, (unit * kg_ref[...]).astype(jnp.bfloat16)


def score_kernel(
    core_ref, qn_ref, g_ref, ck_ref, cv_ref, pkv_ref, qg_ref, kg_ref,
    ds_hbm, dck_ref, dcv_ref, keep_ref, send_ref, gain_ref,
    p_s, ds_s, out_sem,
):
    stores = [pltpu.make_async_copy(ds_s.at[h], ds_hbm.at[h], out_sem.at[h]) for h in range(HK)]
    first_core = core_ref[0] == 0
    key = lax.broadcasted_iota(jnp.int32, (TOK, 2 * TOK), 0)
    slot = lax.rem(lax.broadcasted_iota(jnp.int32, (TOK, 2 * TOK), 1), TOK)
    seen = key <= slot
    qgain = jnp.zeros((8, HD), jnp.float32)
    kgain = jnp.zeros((8, HD), jnp.float32)
    for h in range(HK):
        cols = pl.ds(h * HD, HD)
        pk, pv = unmix(pkv_ref[:, :, cols].astype(jnp.float32))
        unit, inverse, kn = all_keys(pk, ck_ref[:, cols], kg_ref)
        v = jnp.concatenate([pv.astype(jnp.bfloat16), cv_ref[:, cols]], axis=0)
        for pair in range(PER // 2):
            span = pl.ds(pair * 2 * TOK, 2 * TOK)
            rows = pl.ds((h * PER + pair * 2) * TOK, 2 * TOK)
            expo = jnp.exp2(dot(kn, qn_ref[rows, :], NT) * (SCALE * LOG2E))
            expo = jnp.concatenate([expo[:TOK], jnp.where(seen, expo[TOK:], 0.0)], axis=0)
            dprob = dot(v, g_ref[rows, :], NT)
            inv = 1.0 / jnp.sum(expo, axis=0, keepdims=True)
            delta = jnp.sum(expo * dprob, axis=0, keepdims=True) * inv
            prob = expo * inv
            p_s[h, :, span] = prob.astype(jnp.bfloat16)
            ds_s[h, :, span] = (prob * (dprob - delta)).astype(jnp.bfloat16)
        ds_s[h, :, QUERIES:] = kn
        stores[h].start()
        rows = pl.ds(h * QUERIES, QUERIES)
        dv = dot(p_s[h], g_ref[rows, :], NN)
        dk = dot(ds_s[h, :, :QUERIES], qn_ref[rows, :], NN) * SCALE
        qgain += rows_eight(dk * kn.astype(jnp.float32))
        kgain += rows_eight(dk * unit)
        dck_ref[:, cols] = back_of(dk[TOK:], unit[TOK:], inverse[TOK:], kg_ref[...]).astype(jnp.bfloat16)
        dcv_ref[:, cols] = dv[TOK:].astype(jnp.bfloat16)
        zero, one = mix(dk[:TOK], dv[:TOK])
        keep_ref[:, :, cols] = jnp.where(first_core, zero, one).astype(jnp.bfloat16)
        send_ref[:, :, cols] = jnp.where(first_core, one, zero).astype(jnp.bfloat16)
    rows = [jnp.sum(qgain, axis=0, keepdims=True) / qg_ref[...], jnp.sum(kgain, axis=0, keepdims=True)]
    gain_ref[...] = jnp.broadcast_to(jnp.concatenate(rows, axis=0)[None], gain_ref.shape)
    for copy in stores:
        copy.wait()


VMEM = pl.BlockSpec(memory_space=pltpu.VMEM)
ANY = pl.BlockSpec(memory_space=pl.ANY)


def scores(core, qn, g, comp_key, comp_value, prompt, q_gain, k_gain):
    half = jax.ShapeDtypeStruct((PLACES, 8, HK * HD), jnp.bfloat16)
    narrow = jax.ShapeDtypeStruct((TOK, HK * HD), jnp.bfloat16)
    return pl.pallas_call(
        score_kernel,
        in_specs=[pl.BlockSpec(memory_space=pltpu.SMEM)] + [VMEM] * 7,
        out_specs=[ANY] + [VMEM] * 5,
        out_shape=[
            jax.ShapeDtypeStruct((HK, 2 * TOK, QUERIES + HD), jnp.bfloat16),
            narrow,
            narrow,
            half,
            half,
            jax.ShapeDtypeStruct((REPLICAS, 2, HD), jnp.float32),
        ],
        scratch_shapes=[
            pltpu.VMEM((HK, 2 * TOK, QUERIES), jnp.bfloat16),
            pltpu.VMEM((HK, 2 * TOK, QUERIES + HD), jnp.bfloat16),
            pltpu.SemaphoreType.DMA((HK,)),
        ],
        cost_estimate=pl.CostEstimate(
            flops=8 * 2 * HQ * TOK * TOK * HD, bytes_accessed=5 << 20, transcendentals=2 * HQ * TOK * TOK
        ),
        compiler_params=params(SCORE_MIB),
        name="all_scores",
    )(core, qn, g, comp_key, comp_value, prompt, q_gain, k_gain)


def query_kernel(ds_ref, q_ref, qg_ref, dq_ref):
    kn = ds_ref[0, :, QUERIES:]
    for pair in range(PER // 2):
        dn = dot(ds_ref[0, :, pair * 2 * TOK : (pair + 1) * 2 * TOK], kn, TN) * SCALE
        for half in range(2):
            cols = pl.ds((pair * 2 + half) * HD, HD)
            unit, inverse = unit_of(q_ref[:, cols])
            grad = dn[half * TOK : (half + 1) * TOK]
            dq_ref[:, cols] = back_of(grad, unit, inverse, qg_ref[...]).astype(jnp.bfloat16)


def queries_back(part, ds, query, q_gain, filled):
    heads = HK // 2
    wide = pl.BlockSpec((TOK, PER * HD), lambda h: (0, h + part * heads))
    more = [] if filled is None else [filled]
    return pl.pallas_call(
        query_kernel if filled is None else lambda a, b, c, _, d: query_kernel(a, b, c, d),
        grid=(heads,),
        in_specs=[
            pl.BlockSpec((1, 2 * TOK, QUERIES + HD), lambda h: (h + part * heads, 0, 0)), wide, GAIN,
        ] + [ANY] * len(more),
        out_specs=wide,
        out_shape=jax.ShapeDtypeStruct((TOK, HQ * HD), jnp.bfloat16),
        input_output_aliases={} if filled is None else {3: 0},
        cost_estimate=pl.CostEstimate(
            flops=2 * HQ * TOK * TOK * HD, bytes_accessed=5 << 19, transcendentals=0
        ),
        compiler_params=params(60, "arbitrary"),
        name="query_back",
    )(ds, query, q_gain, *more)


def join_kernel(keep_ref, got_ref, out_ref):
    total = keep_ref[...].astype(jnp.float32) + got_ref[...].astype(jnp.float32)
    out_ref[:, :, : HK * HD] = total.astype(jnp.bfloat16)


def join(keep, got):
    return pl.pallas_call(
        join_kernel,
        out_shape=jax.ShapeDtypeStruct((PLACES, 8, (HK + 1) * HD), jnp.bfloat16),
        cost_estimate=pl.CostEstimate(flops=1 << 17, bytes_accessed=400 << 10, transcendentals=0),
        compiler_params=params(4),
        name="core_join",
    )(keep, got)


def relay_kernel(arrived_ref, joined_hbm, out_ref):
    both = jnp.sum(arrived_ref[...], axis=0)
    rows = pieces(both[0:1]) + pieces(both[1:2]) + [jnp.zeros((2, HD), jnp.float32)]
    tile = jnp.concatenate(rows, axis=0)[None]
    out_ref[...] = jnp.broadcast_to(tile, out_ref.shape).astype(jnp.bfloat16)


def relay(arrived, joined):
    return pl.pallas_call(
        relay_kernel,
        grid=(1,),
        in_specs=[pl.BlockSpec((REPLICAS, 2, HD), lambda i: (0, 0, 0)), ANY],
        out_specs=pl.BlockSpec((PLACES, 8, HD), lambda i: (0, 0, HK)),
        out_shape=jax.ShapeDtypeStruct(joined.shape, joined.dtype),
        input_output_aliases={1: 0},
        compiler_params=params(4),
        name="gain_relay",
    )(arrived, joined)


def finish_kernel(arrived_ref, key_ref, kg_ref, dk_ref, dv_ref, gq_ref, gk_ref):
    both = jnp.sum(arrived_ref[...].astype(jnp.float32), axis=0)
    for row, ref in ((0, gq_ref), (3, gk_ref)):
        high, middle, low = [both[row + n : row + n + 1, HK * HD :] for n in range(3)]
        ref[...] = high + (middle + low)
    for h in range(HK):
        cols = pl.ds(h * HD, HD)
        unit, inverse = unit_of(key_ref[:, cols])
        grad = both[:SHARD, h * HD : (h + 1) * HD]
        dk_ref[:, cols] = back_of(grad, unit, inverse, kg_ref[...]).astype(jnp.bfloat16)
    dv_ref[...] = both[SHARD:, : HK * HD].astype(jnp.bfloat16)


def finish(arrived, prompt_key, k_gain):
    out = jax.ShapeDtypeStruct((SHARD, HK * HD), jnp.bfloat16)
    gain = jax.ShapeDtypeStruct((1, HD), jnp.float32)
    return pl.pallas_call(
        finish_kernel,
        out_shape=[out, out, gain, gain],
        cost_estimate=pl.CostEstimate(flops=1 << 20, bytes_accessed=300 << 10, transcendentals=0),
        compiler_params=params(4),
        name="prompt_back",
    )(arrived, prompt_key, k_gain)


def exchange(x, axes):
    return lax.all_to_all(x, axes, split_axis=0, concat_axis=0, tiled=True)


def local(query, comp_key, comp_value, prompt_key, prompt_value, d_out, q_gain, k_gain, lengths):
    q_gain, k_gain = q_gain.reshape(1, HD), k_gain.reshape(1, HD)
    core = lax.axis_index(CORE).reshape(1)
    prompt = exchange(pack(prompt_key, prompt_value), GROUP)
    qn, g = own(lengths, query, d_out, q_gain)
    ds, dck, dcv, keep, send, gains = scores(core, qn, g, comp_key, comp_value, prompt, q_gain, k_gain)
    gains = exchange(gains, DP_CORE)
    joined = join(keep, lax.ppermute(send, CORE, [(0, 1), (1, 0)]))
    dq = queries_back(0, ds, query, q_gain, None)
    gains, dq = lax.optimization_barrier((gains, dq))
    dq = queries_back(1, ds, query, q_gain, dq)
    dpk, dpv, gain_q, gain_k = finish(exchange(relay(gains, joined), PLACE), prompt_key, k_gain)
    return (dq, dck, dcv, dpk, dpv, gain_q.reshape(HD), gain_k.reshape(HD))


def solution(mesh):
    finer = Mesh(
        mesh.devices.reshape(12, 2, 4, 4, 2), ("dp_0", "dp_1", "group_0", "group_1", "group_2")
    )
    rows = P(DP_GROUP, None)
    return jax.shard_map(
        local,
        mesh=finer,
        in_specs=(rows, rows, rows, rows, rows, rows, P(), P(), P(DP_GROUP)),
        out_specs=(rows, rows, rows, rows, rows, P(), P()),
        check_vma=False,
    )
```

```python
import functools

import jax
import jax.numpy as jnp
from jax import lax
from jax.experimental import pallas as pl
from jax.experimental.pallas import tpu as pltpu
from jax.sharding import Mesh
from jax.sharding import PartitionSpec as P

HD = 128
HQ = 32
HK = 4
PER = HQ // HK
TOK = 128
SHARD = 4
PEERS = 32
PLACES = PEERS // 2
REPLICAS = 48
SCORE_MIB = 51
EPS = 1e-06
SCALE = HD ** (-0.5)
LOG2E = 1.4426950408889634
GROUP = ("group_0", "group_1", "group_2")
CORE = "group_2"
PLACE = ("group_0", "group_1")
DP_CORE = ("dp_0", "dp_1", "group_2")
DP_GROUP = ("dp_0", "dp_1", "group_0", "group_1", "group_2")
NT = (((1,), (1,)), ((), ()))
TN = (((0,), (0,)), ((), ()))
NN = (((1,), (0,)), ((), ()))


def dot(a, b, dims):
    return lax.dot_general(a, b, dims, preferred_element_type=jnp.float32)


def unit_of(x):
    wide = x.astype(jnp.float32)
    inverse = lax.rsqrt(jnp.mean(wide * wide, axis=-1, keepdims=True) + EPS)
    return wide * inverse, inverse


def back_of(grad, unit, inverse, gain):
    scaled = grad * gain
    return inverse * (scaled - unit * jnp.mean(scaled * unit, axis=-1, keepdims=True))


def rows_eight(x):
    return jnp.sum(x.reshape(x.shape[0] // 8, 8, x.shape[1]), axis=0)


def unmix(mixed):
    pairs = mixed.reshape(PEERS // 2, 2, 8, HD)
    even, odd = pairs[:, 0], pairs[:, 1]
    low = lax.broadcasted_iota(jnp.int32, even.shape, 1) < SHARD
    first = jnp.where(low, even, pltpu.roll(odd, SHARD, 1))
    second = jnp.where(low, pltpu.roll(even, SHARD, 1), odd)
    return first.reshape(TOK, HD), second.reshape(TOK, HD)


def mix(first, second):
    one = first.reshape(PEERS // 2, 8, HD)
    two = second.reshape(PEERS // 2, 8, HD)
    low = lax.broadcasted_iota(jnp.int32, one.shape, 1) < SHARD
    even = jnp.where(low, one, pltpu.roll(two, SHARD, 1))
    odd = jnp.where(low, pltpu.roll(one, SHARD, 1), two)
    return even, odd


def pieces(x):
    high = x.astype(jnp.bfloat16).astype(jnp.float32)
    middle = (x - high).astype(jnp.bfloat16).astype(jnp.float32)
    return [high, middle, x - high - middle]


def params(mib, *semantics):
    return pltpu.CompilerParams(vmem_limit_bytes=int(mib * 2**20), dimension_semantics=semantics or None)


def pack_kernel(key_ref, value_ref, out_ref):
    own = jnp.concatenate([key_ref[...].astype(jnp.float32), value_ref[...].astype(jnp.float32)], axis=0)
    out_ref[...] = jnp.broadcast_to(own.astype(jnp.bfloat16)[None], out_ref.shape)


def pack(prompt_key, prompt_value):
    return pl.pallas_call(
        pack_kernel,
        out_shape=jax.ShapeDtypeStruct((PEERS, 8, HK * HD), jnp.bfloat16),
        compiler_params=params(60),
        name="prompt_pack",
    )(prompt_key, prompt_value)


def own_kernel(len_ref, q_ref, do_ref, qg_ref, qn_ref, g_ref):
    live = lax.broadcasted_iota(jnp.int32, (TOK, HD), 0) < len_ref[0]
    for j in range(PER):
        cols, rows = pl.ds(j * HD, HD), pl.ds(j * TOK, TOK)
        qunit, _ = unit_of(q_ref[:, cols])
        qn_ref[rows, :] = (qunit * (qg_ref[...] * (SCALE * LOG2E))).astype(jnp.bfloat16)
        g_ref[rows, :] = jnp.where(live, do_ref[:, cols].astype(jnp.float32), 0.0).astype(jnp.bfloat16)


QUERIES = PER * TOK
WIDE = pl.BlockSpec((TOK, PER * HD), lambda h, *_: (0, h))
NARROW = pl.BlockSpec((TOK, HD), lambda h, *_: (0, h))
MIXED = pl.BlockSpec((PEERS, 8, HD), lambda h, *_: (0, 0, h))
GAIN = pl.BlockSpec((1, HD), lambda h, *_: (0, 0))
STACK = pl.BlockSpec((QUERIES, HD), lambda h, *_: (h, 0))


def per_head(rows, columns):
    return pl.BlockSpec((1, rows, columns), lambda h, *_: (h, 0, 0))


def own(lengths, query, d_out, q_gain):
    stacked = jax.ShapeDtypeStruct((HQ * TOK, HD), jnp.bfloat16)
    return pl.pallas_call(
        own_kernel,
        grid_spec=pltpu.PrefetchScalarGridSpec(
            num_scalar_prefetch=1,
            grid=(HK,),
            in_specs=[WIDE, WIDE, GAIN],
            out_specs=[STACK, STACK],
        ),
        out_shape=[stacked, stacked],
        cost_estimate=pl.CostEstimate(flops=1 << 24, bytes_accessed=4 << 20, transcendentals=HQ * TOK),
        compiler_params=params(24, "arbitrary"),
        name="own_norms",
    )(lengths, query, d_out, q_gain)


def all_keys(pk, ck, kg_ref):
    raw = jnp.concatenate([pk, ck.astype(jnp.float32)], axis=0)
    unit, inverse = unit_of(raw)
    return unit, inverse, (unit * kg_ref[...]).astype(jnp.bfloat16)


def score_kernel(
    core_ref, qn_ref, g_ref, ck_ref, cv_ref, pkv_ref, qg_ref, kg_ref,
    ds_hbm, dck_ref, dcv_ref, keep_ref, send_ref, gain_ref,
    p_s, ds_s, out_sem,
):
    stores = [pltpu.make_async_copy(ds_s.at[h], ds_hbm.at[h], out_sem.at[h]) for h in range(HK)]
    first_core = core_ref[0] == 0
    key = lax.broadcasted_iota(jnp.int32, (TOK, 2 * TOK), 0)
    slot = lax.rem(lax.broadcasted_iota(jnp.int32, (TOK, 2 * TOK), 1), TOK)
    seen = key <= slot
    qgain = jnp.zeros((8, HD), jnp.float32)
    kgain = jnp.zeros((8, HD), jnp.float32)
    for h in range(HK):
        cols = pl.ds(h * HD, HD)
        pk, pv = unmix(pkv_ref[:, :, cols].astype(jnp.float32))
        unit, inverse, kn = all_keys(pk, ck_ref[:, cols], kg_ref)
        v = jnp.concatenate([pv.astype(jnp.bfloat16), cv_ref[:, cols]], axis=0)
        for pair in range(PER // 2):
            span = pl.ds(pair * 2 * TOK, 2 * TOK)
            rows = pl.ds((h * PER + pair * 2) * TOK, 2 * TOK)
            expo = jnp.exp2(dot(kn, qn_ref[rows, :], NT))
            expo = jnp.concatenate([expo[:TOK], jnp.where(seen, expo[TOK:], 0.0)], axis=0)
            dprob = dot(v, g_ref[rows, :], NT)
            inv = 1.0 / jnp.sum(expo, axis=0, keepdims=True)
            delta = jnp.sum(expo * dprob, axis=0, keepdims=True) * inv
            prob = expo * inv
            p_s[h, :, span] = prob.astype(jnp.bfloat16)
            ds_s[h, :, span] = (prob * (dprob - delta)).astype(jnp.bfloat16)
        ds_s[h, :, QUERIES:] = kn
        stores[h].start()
        rows = pl.ds(h * QUERIES, QUERIES)
        dv = dot(p_s[h], g_ref[rows, :], NN)
        dk = dot(ds_s[h, :, :QUERIES], qn_ref[rows, :], NN) * (1 / LOG2E)
        qgain += rows_eight(dk * kn.astype(jnp.float32))
        kgain += rows_eight(dk * unit)
        dck_ref[:, cols] = back_of(dk[TOK:], unit[TOK:], inverse[TOK:], kg_ref[...]).astype(jnp.bfloat16)
        dcv_ref[:, cols] = dv[TOK:].astype(jnp.bfloat16)
        zero, one = mix(dk[:TOK], dv[:TOK])
        keep_ref[:, :, cols] = jnp.where(first_core, zero, one).astype(jnp.bfloat16)
        send_ref[:, :, cols] = jnp.where(first_core, one, zero).astype(jnp.bfloat16)
    rows = [jnp.sum(qgain, axis=0, keepdims=True) / qg_ref[...], jnp.sum(kgain, axis=0, keepdims=True)]
    gain_ref[...] = jnp.broadcast_to(jnp.concatenate(rows, axis=0)[None], gain_ref.shape)
    for copy in stores:
        copy.wait()


VMEM = pl.BlockSpec(memory_space=pltpu.VMEM)
ANY = pl.BlockSpec(memory_space=pl.ANY)


def scores(core, qn, g, comp_key, comp_value, prompt, q_gain, k_gain):
    half = jax.ShapeDtypeStruct((PLACES, 8, HK * HD), jnp.bfloat16)
    narrow = jax.ShapeDtypeStruct((TOK, HK * HD), jnp.bfloat16)
    return pl.pallas_call(
        score_kernel,
        in_specs=[pl.BlockSpec(memory_space=pltpu.SMEM)] + [VMEM] * 7,
        out_specs=[ANY] + [VMEM] * 5,
        out_shape=[
            jax.ShapeDtypeStruct((HK, 2 * TOK, QUERIES + HD), jnp.bfloat16),
            narrow,
            narrow,
            half,
            half,
            jax.ShapeDtypeStruct((REPLICAS, 2, HD), jnp.float32),
        ],
        scratch_shapes=[
            pltpu.VMEM((HK, 2 * TOK, QUERIES), jnp.bfloat16),
            pltpu.VMEM((HK, 2 * TOK, QUERIES + HD), jnp.bfloat16),
            pltpu.SemaphoreType.DMA((HK,)),
        ],
        cost_estimate=pl.CostEstimate(
            flops=8 * 2 * HQ * TOK * TOK * HD, bytes_accessed=5 << 20, transcendentals=2 * HQ * TOK * TOK
        ),
        compiler_params=pltpu.CompilerParams(
            vmem_limit_bytes=SCORE_MIB << 20
        ),
        name="all_scores",
    )(core, qn, g, comp_key, comp_value, prompt, q_gain, k_gain)


def query_kernel(ds_ref, q_ref, qg_ref, dq_ref):
    kn = ds_ref[0, :, QUERIES:]
    for pair in range(PER // 2):
        dn = dot(ds_ref[0, :, pair * 2 * TOK : (pair + 1) * 2 * TOK], kn, TN) * SCALE
        for half in range(2):
            cols = pl.ds((pair * 2 + half) * HD, HD)
            unit, inverse = unit_of(q_ref[:, cols])
            grad = dn[half * TOK : (half + 1) * TOK]
            dq_ref[:, cols] = back_of(grad, unit, inverse, qg_ref[...]).astype(jnp.bfloat16)


def queries_back(part, ds, query, q_gain, filled):
    heads = HK // 2
    wide = pl.BlockSpec((TOK, PER * HD), lambda h: (0, h + part * heads))
    more = [] if filled is None else [filled]
    return pl.pallas_call(
        query_kernel if filled is None else lambda a, b, c, _, d: query_kernel(a, b, c, d),
        grid=(heads,),
        in_specs=[
            pl.BlockSpec((1, 2 * TOK, QUERIES + HD), lambda h: (h + part * heads, 0, 0)), wide, GAIN,
        ] + [ANY] * len(more),
        out_specs=wide,
        out_shape=jax.ShapeDtypeStruct((TOK, HQ * HD), jnp.bfloat16),
        input_output_aliases={} if filled is None else {3: 0},
        cost_estimate=pl.CostEstimate(
            flops=2 * HQ * TOK * TOK * HD, bytes_accessed=5 << 19, transcendentals=0
        ),
        compiler_params=params(60, "arbitrary"),
        name="query_back",
    )(ds, query, q_gain, *more)


def join_kernel(keep_ref, got_ref, out_ref):
    total = keep_ref[...].astype(jnp.float32) + got_ref[...].astype(jnp.float32)
    out_ref[:, :, : HK * HD] = total.astype(jnp.bfloat16)


def join(keep, got):
    return pl.pallas_call(
        join_kernel,
        out_shape=jax.ShapeDtypeStruct((PLACES, 8, (HK + 1) * HD), jnp.bfloat16),
        cost_estimate=pl.CostEstimate(flops=1 << 17, bytes_accessed=400 << 10, transcendentals=0),
        compiler_params=params(4),
        name="core_join",
    )(keep, got)


def relay_kernel(arrived_ref, joined_hbm, out_ref):
    both = jnp.sum(arrived_ref[...], axis=0)
    rows = pieces(both[0:1]) + pieces(both[1:2]) + [jnp.zeros((2, HD), jnp.float32)]
    tile = jnp.concatenate(rows, axis=0)[None]
    out_ref[...] = jnp.broadcast_to(tile, out_ref.shape).astype(jnp.bfloat16)


def relay(arrived, joined):
    return pl.pallas_call(
        relay_kernel,
        grid=(1,),
        in_specs=[pl.BlockSpec((REPLICAS, 2, HD), lambda i: (0, 0, 0)), ANY],
        out_specs=pl.BlockSpec((PLACES, 8, HD), lambda i: (0, 0, HK)),
        out_shape=jax.ShapeDtypeStruct(joined.shape, joined.dtype),
        input_output_aliases={1: 0},
        compiler_params=params(4),
        name="gain_relay",
    )(arrived, joined)


def finish_kernel(arrived_ref, key_ref, kg_ref, dk_ref, dv_ref, gq_ref, gk_ref):
    both = jnp.sum(arrived_ref[...].astype(jnp.float32), axis=0)
    for row, ref in ((0, gq_ref), (3, gk_ref)):
        high, middle, low = [both[row + n : row + n + 1, HK * HD :] for n in range(3)]
        ref[...] = high + (middle + low)
    for h in range(HK):
        cols = pl.ds(h * HD, HD)
        unit, inverse = unit_of(key_ref[:, cols])
        grad = both[:SHARD, h * HD : (h + 1) * HD]
        dk_ref[:, cols] = back_of(grad, unit, inverse, kg_ref[...]).astype(jnp.bfloat16)
    dv_ref[...] = both[SHARD:, : HK * HD].astype(jnp.bfloat16)


def finish(arrived, prompt_key, k_gain):
    out = jax.ShapeDtypeStruct((SHARD, HK * HD), jnp.bfloat16)
    gain = jax.ShapeDtypeStruct((1, HD), jnp.float32)
    return pl.pallas_call(
        finish_kernel,
        out_shape=[out, out, gain, gain],
        cost_estimate=pl.CostEstimate(flops=1 << 20, bytes_accessed=300 << 10, transcendentals=0),
        compiler_params=params(4),
        name="prompt_back",
    )(arrived, prompt_key, k_gain)


def exchange(x, axes):
    return lax.all_to_all(x, axes, split_axis=0, concat_axis=0, tiled=True)


def local(query, comp_key, comp_value, prompt_key, prompt_value, d_out, q_gain, k_gain, lengths):
    q_gain, k_gain = q_gain.reshape(1, HD), k_gain.reshape(1, HD)
    core = lax.axis_index(CORE).reshape(1)
    prompt = exchange(pack(prompt_key, prompt_value), GROUP)
    qn, g = own(lengths, query, d_out, q_gain)
    ds, dck, dcv, keep, send, gains = scores(core, qn, g, comp_key, comp_value, prompt, q_gain, k_gain)
    gains = exchange(gains, DP_CORE)
    joined = join(keep, lax.ppermute(send, CORE, [(0, 1), (1, 0)]))
    dq = queries_back(0, ds, query, q_gain, None)
    gains, dq = lax.optimization_barrier((gains, dq))
    dq = queries_back(1, ds, query, q_gain, dq)
    dpk, dpv, gain_q, gain_k = finish(exchange(relay(gains, joined), PLACE), prompt_key, k_gain)
    return (dq, dck, dcv, dpk, dpv, gain_q.reshape(HD), gain_k.reshape(HD))


def solution(mesh):
    finer = Mesh(
        mesh.devices.reshape(12, 2, 4, 4, 2), ("dp_0", "dp_1", "group_0", "group_1", "group_2")
    )
    rows = P(DP_GROUP, None)
    return jax.shard_map(
        local,
        mesh=finer,
        in_specs=(rows, rows, rows, rows, rows, rows, P(), P(), P(DP_GROUP)),
        out_specs=(rows, rows, rows, rows, rows, P(), P()),
        check_vma=False,
    )
```

```python
import functools

import jax
import jax.numpy as jnp
from jax import lax
from jax.experimental import pallas as pl
from jax.experimental.pallas import tpu as pltpu
from jax.sharding import Mesh
from jax.sharding import PartitionSpec as P

HD = 128
HQ = 32
HK = 4
PER = HQ // HK
TOK = 128
SHARD = 4
PEERS = 32
PLACES = PEERS // 2
REPLICAS = 48
SCORE_MIB = 51
EPS = 1e-06
SCALE = HD ** (-0.5)
LOG2E = 1.4426950408889634
GROUP = ("group_0", "group_1", "group_2")
CORE = "group_2"
PLACE = ("group_0", "group_1")
DP_CORE = ("dp_0", "dp_1", "group_2")
DP_GROUP = ("dp_0", "dp_1", "group_0", "group_1", "group_2")
NT = (((1,), (1,)), ((), ()))
TN = (((0,), (0,)), ((), ()))
NN = (((1,), (0,)), ((), ()))


def dot(a, b, dims):
    return lax.dot_general(a, b, dims, preferred_element_type=jnp.float32)


def unit_of(x):
    wide = x.astype(jnp.float32)
    inverse = lax.rsqrt(jnp.mean(wide * wide, axis=-1, keepdims=True) + EPS)
    return wide * inverse, inverse


def back_of(grad, unit, inverse, gain):
    scaled = grad * gain
    return inverse * (scaled - unit * jnp.mean(scaled * unit, axis=-1, keepdims=True))


def rows_eight(x):
    return jnp.sum(x.reshape(x.shape[0] // 8, 8, x.shape[1]), axis=0)


def unmix(mixed):
    pairs = mixed.reshape(PEERS // 2, 2, 8, HD)
    even, odd = pairs[:, 0], pairs[:, 1]
    low = lax.broadcasted_iota(jnp.int32, even.shape, 1) < SHARD
    first = jnp.where(low, even, pltpu.roll(odd, SHARD, 1))
    second = jnp.where(low, pltpu.roll(even, SHARD, 1), odd)
    return first.reshape(TOK, HD), second.reshape(TOK, HD)


def mix(first, second):
    one = first.reshape(PEERS // 2, 8, HD)
    two = second.reshape(PEERS // 2, 8, HD)
    low = lax.broadcasted_iota(jnp.int32, one.shape, 1) < SHARD
    even = jnp.where(low, one, pltpu.roll(two, SHARD, 1))
    odd = jnp.where(low, pltpu.roll(one, SHARD, 1), two)
    return even, odd


def pieces(x):
    high = x.astype(jnp.bfloat16).astype(jnp.float32)
    middle = (x - high).astype(jnp.bfloat16).astype(jnp.float32)
    return [high, middle, x - high - middle]


def params(mib, *semantics):
    return pltpu.CompilerParams(vmem_limit_bytes=int(mib * 2**20), dimension_semantics=semantics or None)


def pack_kernel(key_ref, value_ref, out_ref):
    own = jnp.concatenate([key_ref[...].astype(jnp.float32), value_ref[...].astype(jnp.float32)], axis=0)
    out_ref[...] = jnp.broadcast_to(own.astype(jnp.bfloat16)[None], out_ref.shape)


def pack(prompt_key, prompt_value):
    return pl.pallas_call(
        pack_kernel,
        out_shape=jax.ShapeDtypeStruct((PEERS, 8, HK * HD), jnp.bfloat16),
        compiler_params=params(60),
        name="prompt_pack",
    )(prompt_key, prompt_value)


def own_kernel(len_ref, q_ref, do_ref, qg_ref, qn_ref, g_ref):
    live = lax.broadcasted_iota(jnp.int32, (TOK, HD), 0) < len_ref[0]
    for j in range(PER):
        cols, rows = pl.ds(j * HD, HD), pl.ds(j * TOK, TOK)
        qunit, _ = unit_of(q_ref[:, cols])
        qn_ref[rows, :] = (qunit * (qg_ref[...] * (SCALE * LOG2E))).astype(jnp.bfloat16)
        g_ref[rows, :] = jnp.where(live, do_ref[:, cols].astype(jnp.float32), 0.0).astype(jnp.bfloat16)


QUERIES = PER * TOK
WIDE = pl.BlockSpec((TOK, PER * HD), lambda h, *_: (0, h))
NARROW = pl.BlockSpec((TOK, HD), lambda h, *_: (0, h))
MIXED = pl.BlockSpec((PEERS, 8, HD), lambda h, *_: (0, 0, h))
GAIN = pl.BlockSpec((1, HD), lambda h, *_: (0, 0))
STACK = pl.BlockSpec((QUERIES, HD), lambda h, *_: (h, 0))


def per_head(rows, columns):
    return pl.BlockSpec((1, rows, columns), lambda h, *_: (h, 0, 0))


def own(lengths, query, d_out, q_gain):
    stacked = jax.ShapeDtypeStruct((HQ * TOK, HD), jnp.bfloat16)
    return pl.pallas_call(
        own_kernel,
        grid_spec=pltpu.PrefetchScalarGridSpec(
            num_scalar_prefetch=1,
            grid=(HK,),
            in_specs=[WIDE, WIDE, GAIN],
            out_specs=[STACK, STACK],
        ),
        out_shape=[stacked, stacked],
        cost_estimate=pl.CostEstimate(flops=1 << 24, bytes_accessed=4 << 20, transcendentals=HQ * TOK),
        compiler_params=params(24, "arbitrary"),
        name="own_norms",
    )(lengths, query, d_out, q_gain)


def all_keys(pk, ck, kg_ref):
    raw = jnp.concatenate([pk, ck.astype(jnp.float32)], axis=0)
    unit, inverse = unit_of(raw)
    return unit, inverse, (unit * kg_ref[...]).astype(jnp.bfloat16)


def score_kernel(
    core_ref, qn_ref, g_ref, ck_ref, cv_ref, pkv_ref, qg_ref, kg_ref,
    ds_hbm, dck_ref, dcv_ref, keep_ref, send_ref, gain_ref,
    p_s, ds_s, out_sem,
):
    stores = [pltpu.make_async_copy(ds_s.at[h], ds_hbm.at[h], out_sem.at[h]) for h in range(HK)]
    first_core = core_ref[0] == 0
    key = lax.broadcasted_iota(jnp.int32, (TOK, 2 * TOK), 0)
    slot = lax.rem(lax.broadcasted_iota(jnp.int32, (TOK, 2 * TOK), 1), TOK)
    seen = key <= slot
    qgain = jnp.zeros((8, HD), jnp.float32)
    kgain = jnp.zeros((8, HD), jnp.float32)
    for h in range(HK):
        cols = pl.ds(h * HD, HD)
        pk, pv = unmix(pkv_ref[:, :, cols].astype(jnp.float32))
        unit, inverse, kn = all_keys(pk, ck_ref[:, cols], kg_ref)
        v = jnp.concatenate([pv.astype(jnp.bfloat16), cv_ref[:, cols]], axis=0)
        for pair in range(PER // 2):
            span = pl.ds(pair * 2 * TOK, 2 * TOK)
            rows = pl.ds((h * PER + pair * 2) * TOK, 2 * TOK)
            expo = jnp.exp2(dot(kn, qn_ref[rows, :], NT))
            expo = jnp.concatenate([expo[:TOK], jnp.where(seen, expo[TOK:], 0.0)], axis=0)
            dprob = dot(v, g_ref[rows, :], NT)
            inv = 1.0 / jnp.sum(expo, axis=0, keepdims=True)
            delta = jnp.sum(expo * dprob, axis=0, keepdims=True) * inv
            prob = expo * inv
            p_s[h, :, span] = prob.astype(jnp.bfloat16)
            ds_s[h, :, span] = (prob * (dprob - delta)).astype(jnp.bfloat16)
        ds_s[h, :, QUERIES:] = kn
        stores[h].start()
        rows = pl.ds(h * QUERIES, QUERIES)
        dv = dot(p_s[h], g_ref[rows, :], NN)
        dk = dot(ds_s[h, :, :QUERIES], qn_ref[rows, :], NN) * (1 / LOG2E)
        qgain += rows_eight(dk * kn.astype(jnp.float32))
        kgain += rows_eight(dk * unit)
        dck_ref[:, cols] = back_of(dk[TOK:], unit[TOK:], inverse[TOK:], kg_ref[...]).astype(jnp.bfloat16)
        dcv_ref[:, cols] = dv[TOK:].astype(jnp.bfloat16)
        zero, one = mix(dk[:TOK], dv[:TOK])
        keep_ref[:, :, cols] = jnp.where(first_core, zero, one).astype(jnp.bfloat16)
        send_ref[:, :, cols] = jnp.where(first_core, one, zero).astype(jnp.bfloat16)
    rows = [jnp.sum(qgain, axis=0, keepdims=True) / qg_ref[...], jnp.sum(kgain, axis=0, keepdims=True)]
    gain_ref[...] = jnp.broadcast_to(jnp.concatenate(rows, axis=0)[None], gain_ref.shape)
    for copy in stores:
        copy.wait()


VMEM = pl.BlockSpec(memory_space=pltpu.VMEM)
ANY = pl.BlockSpec(memory_space=pl.ANY)


def scores(core, qn, g, comp_key, comp_value, prompt, q_gain, k_gain):
    half = jax.ShapeDtypeStruct((PLACES, 8, HK * HD), jnp.bfloat16)
    narrow = jax.ShapeDtypeStruct((TOK, HK * HD), jnp.bfloat16)
    return pl.pallas_call(
        score_kernel,
        in_specs=[pl.BlockSpec(memory_space=pltpu.SMEM)] + [VMEM] * 7,
        out_specs=[ANY] + [VMEM] * 5,
        out_shape=[
            jax.ShapeDtypeStruct((HK, 2 * TOK, QUERIES + HD), jnp.bfloat16),
            narrow,
            narrow,
            half,
            half,
            jax.ShapeDtypeStruct((REPLICAS, 2, HD), jnp.float32),
        ],
        scratch_shapes=[
            pltpu.VMEM((HK, 2 * TOK, QUERIES), jnp.bfloat16),
            pltpu.VMEM((HK, 2 * TOK, QUERIES + HD), jnp.bfloat16),
            pltpu.SemaphoreType.DMA((HK,)),
        ],
        cost_estimate=pl.CostEstimate(
            flops=8 * 2 * HQ * TOK * TOK * HD, bytes_accessed=5 << 20, transcendentals=2 * HQ * TOK * TOK
        ),
        compiler_params=pltpu.CompilerParams(
            vmem_limit_bytes=SCORE_MIB << 20
        ),
        name="all_scores",
    )(core, qn, g, comp_key, comp_value, prompt, q_gain, k_gain)


def query_kernel(ds_ref, q_ref, qg_ref, dq_ref):
    kn = ds_ref[0, :, QUERIES:]
    for pair in range(PER // 2):
        dn = dot(ds_ref[0, :, pair * 2 * TOK : (pair + 1) * 2 * TOK], kn, TN) * SCALE
        for half in range(2):
            cols = pl.ds((pair * 2 + half) * HD, HD)
            unit, inverse = unit_of(q_ref[:, cols])
            grad = dn[half * TOK : (half + 1) * TOK]
            dq_ref[:, cols] = back_of(grad, unit, inverse, qg_ref[...]).astype(jnp.bfloat16)


def queries_back(ds, query, q_gain):
    return pl.pallas_call(
        query_kernel,
        grid=(HK,),
        in_specs=[per_head(2 * TOK, QUERIES + HD), WIDE, GAIN],
        out_specs=WIDE,
        out_shape=jax.ShapeDtypeStruct((TOK, HQ * HD), jnp.bfloat16),
        cost_estimate=pl.CostEstimate(
            flops=2 * 2 * HQ * TOK * TOK * HD, bytes_accessed=5 << 20, transcendentals=0
        ),
        compiler_params=params(60, "arbitrary"),
        name="query_back",
    )(ds, query, q_gain)


def join_kernel(keep_ref, got_ref, out_ref):
    total = keep_ref[...].astype(jnp.float32) + got_ref[...].astype(jnp.float32)
    out_ref[:, :, : HK * HD] = total.astype(jnp.bfloat16)


def join(keep, got):
    return pl.pallas_call(
        join_kernel,
        out_shape=jax.ShapeDtypeStruct((PLACES, 8, (HK + 1) * HD), jnp.bfloat16),
        cost_estimate=pl.CostEstimate(flops=1 << 17, bytes_accessed=400 << 10, transcendentals=0),
        compiler_params=params(4),
        name="core_join",
    )(keep, got)


def relay_kernel(arrived_ref, joined_hbm, out_ref):
    both = jnp.sum(arrived_ref[...], axis=0)
    rows = pieces(both[0:1]) + pieces(both[1:2]) + [jnp.zeros((2, HD), jnp.float32)]
    tile = jnp.concatenate(rows, axis=0)[None]
    out_ref[...] = jnp.broadcast_to(tile, out_ref.shape).astype(jnp.bfloat16)


def relay(arrived, joined):
    return pl.pallas_call(
        relay_kernel,
        grid=(1,),
        in_specs=[pl.BlockSpec((REPLICAS, 2, HD), lambda i: (0, 0, 0)), ANY],
        out_specs=pl.BlockSpec((PLACES, 8, HD), lambda i: (0, 0, HK)),
        out_shape=jax.ShapeDtypeStruct(joined.shape, joined.dtype),
        input_output_aliases={1: 0},
        compiler_params=params(4),
        name="gain_relay",
    )(arrived, joined)


def finish_kernel(arrived_ref, key_ref, kg_ref, dk_ref, dv_ref, gq_ref, gk_ref):
    both = jnp.sum(arrived_ref[...].astype(jnp.float32), axis=0)
    for row, ref in ((0, gq_ref), (3, gk_ref)):
        high, middle, low = [both[row + n : row + n + 1, HK * HD :] for n in range(3)]
        ref[...] = high + (middle + low)
    for h in range(HK):
        cols = pl.ds(h * HD, HD)
        unit, inverse = unit_of(key_ref[:, cols])
        grad = both[:SHARD, h * HD : (h + 1) * HD]
        dk_ref[:, cols] = back_of(grad, unit, inverse, kg_ref[...]).astype(jnp.bfloat16)
    dv_ref[...] = both[SHARD:, : HK * HD].astype(jnp.bfloat16)


def finish(arrived, prompt_key, k_gain):
    out = jax.ShapeDtypeStruct((SHARD, HK * HD), jnp.bfloat16)
    gain = jax.ShapeDtypeStruct((1, HD), jnp.float32)
    return pl.pallas_call(
        finish_kernel,
        out_shape=[out, out, gain, gain],
        cost_estimate=pl.CostEstimate(flops=1 << 20, bytes_accessed=300 << 10, transcendentals=0),
        compiler_params=params(4),
        name="prompt_back",
    )(arrived, prompt_key, k_gain)


def exchange(x, axes):
    return lax.all_to_all(x, axes, split_axis=0, concat_axis=0, tiled=True)


def local(query, comp_key, comp_value, prompt_key, prompt_value, d_out, q_gain, k_gain, lengths):
    q_gain, k_gain = q_gain.reshape(1, HD), k_gain.reshape(1, HD)
    core = lax.axis_index(CORE).reshape(1)
    prompt = exchange(pack(prompt_key, prompt_value), GROUP)
    qn, g = own(lengths, query, d_out, q_gain)
    ds, dck, dcv, keep, send, gains = scores(core, qn, g, comp_key, comp_value, prompt, q_gain, k_gain)
    gains = exchange(gains, DP_CORE)
    joined = join(keep, lax.ppermute(send, CORE, [(0, 1), (1, 0)]))
    dq = queries_back(ds, query, q_gain)
    dpk, dpv, gain_q, gain_k = finish(exchange(relay(gains, joined), PLACE), prompt_key, k_gain)
    return (dq, dck, dcv, dpk, dpv, gain_q.reshape(HD), gain_k.reshape(HD))


def solution(mesh):
    finer = Mesh(
        mesh.devices.reshape(12, 2, 4, 4, 2), ("dp_0", "dp_1", "group_0", "group_1", "group_2")
    )
    rows = P(DP_GROUP, None)
    return jax.shard_map(
        local,
        mesh=finer,
        in_specs=(rows, rows, rows, rows, rows, rows, P(), P(), P(DP_GROUP)),
        out_specs=(rows, rows, rows, rows, rows, P(), P()),
        check_vma=False,
    )
```
